512 devices in a mesh: dp: 2 (over core), row: 8 (over x, z_hi), col: 32 (over y, z_lo).
Axes of the slice: x: 4, y: 8, z: 8 (z_hi: 2, z_lo: 4; z = z_hi * 4 + z_lo), core: 2. Of those that a mesh axis runs over, the one named last changes fastest.
Arguments:
- hidden: bfloat16 [2048, 28672], P(('dp', 'row'), 'col'), may hold values from -0.125 to 0.125
- upstream: bfloat16 [2048, 8192], P('col', ('dp', 'row')), may hold values from -6 to 6
- weight: bfloat16 [28672, 8192], P('col', ('dp', 'row')), may hold values from -0.03125 to 0.03125
Outputs:
- input_grad: bfloat16 [2048, 28672], P(('dp', 'row'), 'col')
- weight_grad: float32 [28672, 8192], P('col', ('dp', 'row'))
The draws below stay inside these ranges and needn't reach their ends.
All inputs are finite; a program needn't handle non-finite values.
Results may differ from the reference program's by a relative error of at most 0.014.
Values may be sent and summed in bfloat16 or wider, within the bound.
A program may use at most 64 MiB of HBM per device.

```python
import jax
import jax.numpy as jnp
from jax import lax

D = 8192
FF = 28672
TOKENS = 2048
N_DP = 2
N_ROW = 8


def strengthened(values, rng, source, target, shards_of, factor):
    def block_of(dim):
        return (jnp.arange(values.shape[dim]) // (values.shape[dim] // shards_of)).reshape((-1,) + (1,) * (values.ndim - 1 - dim))

    near = jax.random.permutation(rng, shards_of)[block_of(target)]
    other_side = (block_of(target) + shards_of // 2) % shards_of
    return jnp.where((block_of(source) == near) | (block_of(source) == other_side), factor * values, values)


def steps_of(stream_key, dims, pieces, smallest, high):
    def one(dim, shards_of):
        heights = jax.random.uniform(jax.random.fold_in(jax.random.fold_in(stream_key, 6), dim), (shards_of,), jnp.float32, smallest / len(pieces), high / len(pieces))
        return jnp.repeat(jnp.exp(heights), dims[dim] // shards_of).reshape((-1,) + (1,) * (len(dims) - dim - 1))

    loudness = one(*pieces[0])
    for cut in pieces[1:]:
        loudness = loudness * one(*cut)
    return loudness


def gaussian(key, shape, spread, most, shards=(), kind=jnp.bfloat16):
    drawn = spread * jax.random.normal(key, shape, jnp.float32)
    if shards:
        drawn = drawn * steps_of(key, shape, shards, -0.22, 0.18)
    return jnp.clip(drawn, -most, most).astype(kind)


def bell_draw_with(key, dims, scale, reach, cuts, heavy, dtype=jnp.bfloat16):
    values = scale * jax.random.normal(key, dims, jnp.float32)
    if cuts:
        values = values * steps_of(key, dims, cuts, -0.22, 0.18)
    return jnp.clip(strengthened(values, jax.random.fold_in(key, 3), *heavy), -reach, reach).astype(dtype)


def setup_inputs(seed: int = 0) -> dict:
    arg_keys = jax.random.split(jax.random.key(seed), 4)
    hidden = gaussian(arg_keys[0], (TOKENS, FF), TOKENS ** -0.5, 0.125, ((0, 16), (1, 32)))
    upstream = bell_draw_with(arg_keys[1], (TOKENS, D), 1.0, 6.0, ((0, 32), (1, 16)), (1, 0, 32, 2.75))
    weight = gaussian(arg_keys[2], (FF, D), FF ** -0.5, 0.03125, ((0, 32), (1, 16)))
    return {"hidden": hidden, "upstream": upstream, "weight": weight}


def reference(hidden, upstream, weight):
    weight_grad = lax.dot_general(hidden, upstream, (((0,), (0,)), ((), ())), preferred_element_type=jnp.float32)
    groups = N_DP * N_ROW
    columns = D // groups
    summed = jnp.zeros((hidden.shape[0], FF), jnp.float32)
    for member in range(groups):
        window = upstream[:, member * columns:(member + 1) * columns]
        slab = weight[:, member * columns:(member + 1) * columns]
        product = lax.dot_general(window, slab, (((1,), (1,)), ((), ())), preferred_element_type=jnp.float32)
        rounded = lax.optimization_barrier(product.astype(jnp.bfloat16))
        summed = summed + rounded.astype(jnp.float32)
    return summed.astype(jnp.bfloat16), weight_grad
```

```python
import jax
import jax.numpy as jnp
from jax import lax
from jax.experimental import pallas as pl
from jax.experimental.pallas import tpu as pltpu
from jax.sharding import Mesh
from jax.sharding import PartitionSpec as P

DP_ROW = ("dp", "x", "zh")
COL = ("y", "zl")
MESH = pl.DeviceIdType.MESH
BF16 = jnp.bfloat16
F32 = jnp.float32


def rows(ref, start, count):
    return ref.at[pl.ds(pl.multiple_of(start, 64), count)]


def done(ref, sem):
    pltpu.make_async_copy(ref, ref, sem).wait()


def kernel(
    hid_in, up_in, w_in, ig_out, dw_out,
    U, UP, H, W, WP, T, c1p, c1m, c2p, c2m, zs, zr, own, igv, dwv,
    s_loc, s_a1, s_yp, s_ym, s_up, s_w, s_bz, s_bxp, s_bxm, s_bfp, s_bfm, s_hd,
    s_c1p, s_c1m, s_c2p, s_c2m, s_z,
    t_u, t_up, t_w, t_h, t_hd, t_c, t_out,
):
    c = lax.axis_index("dp")
    x = lax.axis_index("x")
    h = lax.axis_index("zh")
    y = lax.axis_index("y")
    l = lax.axis_index("zl")
    other = {"dp": 1 - c}
    xp = {"x": lax.rem(x + 1, 4)}
    xm = {"x": lax.rem(x + 3, 4)}
    yp = {"y": lax.rem(y + 1, 8)}
    ym = {"y": lax.rem(y + 7, 8)}
    zo = {"zh": 1 - h}
    line = [l, l + 1 - 2 * lax.rem(l, 2), lax.rem(l + 2, 4), 3 - l]
    mates = [{"zl": k} for k in line[1:]]

    def send(src, dst, t, s, to):
        pltpu.make_async_remote_copy(
            src_ref=src, dst_ref=dst, send_sem=t, recv_sem=s, device_id=to, device_id_type=MESH
        ).start()

    def urow(block, i):
        return (block * 4 + line[i]) * 64

    def hrow(core, xx, hh):
        return (core * 8 + xx * 2 + hh) * 128

    local_up = pltpu.make_async_copy(up_in, rows(U, urow(y, 0), 64), s_loc.at[0])
    local_hid = pltpu.make_async_copy(hid_in, rows(H, hrow(c, x, h), 128), s_loc.at[1])
    local_w = pltpu.make_async_copy(w_in, W, s_loc.at[2])
    local_up.start()
    local_hid.start()
    local_w.start()

    barrier = pltpu.get_barrier_semaphore()
    partners = mates + [yp, ym, xp, xm, zo, other]
    for to in partners:
        pl.semaphore_signal(barrier, inc=1, device_id=to, device_id_type=MESH)
    pl.semaphore_wait(barrier, len(partners))

    local_up.wait()
    mine = rows(U, urow(y, 0), 64)
    for i in range(1, 4):
        send(mine, mine, t_u, s_a1.at[i - 1], mates[i - 1])
    send(mine, mine, t_u, s_yp.at[0], yp)
    send(mine, mine, t_u, s_ym.at[0], ym)

    def to_partner(block, i):
        @pl.when(block // 4 != c)
        def _():
            b4 = lax.rem(block, 4)
            send(rows(U, urow(block, i), 64), rows(UP, (b4 * 4 + line[i]) * 64, 64), t_up, s_up.at[b4], other)

    to_partner(y, 0)

    local_hid.wait()

    def share(xx, hh, part, to, sem):
        piece = rows(H, hrow(c, xx, hh) + part * 64, 64)
        send(piece, piece, t_h, sem, to)

    share(x, h, 0, xp, s_bxp.at[0, 0])
    share(x, h, 1, xm, s_bxm.at[0, 1])
    share(x, h, 1, xp, s_bxp.at[0, 1])
    share(x, h, 0, xm, s_bxm.at[0, 0])

    def hid_across(xx, hh):
        piece = rows(H, hrow(c, xx, hh), 128)
        send(piece, piece, t_hd, s_hd.at[0], other)

    hid_across(x, h)
    local_w.wait()
    send(W, WP, t_w, s_w.at[0], other)

    for i in range(1, 4):
        piece = rows(U, urow(y, i), 64)
        done(piece, s_a1.at[i - 1])
        send(piece, piece, t_u, s_yp.at[i], yp)
        send(piece, piece, t_u, s_ym.at[i], ym)
        to_partner(y, i)
        if i == 1:
            share(x, h, 0, zo, s_bz.at[0])
            share(x, h, 1, zo, s_bz.at[1])
    done(WP, s_w.at[0])

    def quarter(xx, hh, ab):
        return T.at[xx, pl.ds(pl.multiple_of(hh * 128 + ab * 64, 64), 64)]

    sides = (1 - h, h)

    def block_step(delta):
        block = lax.rem(y + delta + 8, 8)
        b4 = lax.rem(block, 4)
        d = lax.rem(b4 - x + 4, 4)

        @pl.when(block // 4 == c)
        def _():
            done(rows(UP, b4 * 256, 256), s_up.at[b4])
            u = rows(U, block * 256, 256)
            up = rows(UP, b4 * 256, 256)
            dims = (((1,), (1,)), ((), ()))
            for n0 in range(0, 896, 256):
                n1 = min(n0 + 256, 896)
                acc = lax.dot_general(u[...], W[n0:n1], dims, preferred_element_type=F32)
                acc += lax.dot_general(up[...], WP[n0:n1], dims, preferred_element_type=F32)
                T[b4, :, n0:n1] = acc.astype(BF16)

            @pl.when(d == 2)
            def _():
                for k in range(2):
                    send(quarter(b4, sides[k], 0), c1p.at[k], t_c, s_c1p.at[k], xp)
                    send(quarter(b4, sides[k], 1), c1m.at[k], t_c, s_c1m.at[k], xm)

            @pl.when(d == 1)
            def _():
                for k in range(2):
                    send(quarter(b4, sides[k], 1), c2p.at[k, 1], t_c, s_c2p.at[k, 1], xp)

            @pl.when(d == 3)
            def _():
                for k in range(2):
                    send(quarter(b4, sides[k], 0), c2m.at[k, 0], t_c, s_c2m.at[k, 0], xm)

    def add_step(delta):
        block = lax.rem(y + delta + 8, 8)
        b4 = lax.rem(block, 4)
        d = lax.rem(b4 - x + 4, 4)
        here = block // 4 == c

        @pl.when(jnp.logical_and(here, d == 1))
        def _():
            for k in range(2):
                done(c1p.at[k], s_c1p.at[k])
                q = quarter(b4, sides[k], 0)
                q[...] = (q[...].astype(F32) + c1p[k].astype(F32)).astype(BF16)
                send(q, c2p.at[k, 0], t_c, s_c2p.at[k, 0], xp)

        @pl.when(jnp.logical_and(here, d == 3))
        def _():
            for k in range(2):
                done(c1m.at[k], s_c1m.at[k])
                q = quarter(b4, sides[k], 1)
                q[...] = (q[...].astype(F32) + c1m[k].astype(F32)).astype(BF16)
                send(q, c2m.at[k, 1], t_c, s_c2m.at[k, 1], xm)

    def sum_step(delta):
        block = lax.rem(y + delta + 8, 8)
        b4 = lax.rem(block, 4)
        d = lax.rem(b4 - x + 4, 4)

        @pl.when(jnp.logical_and(block // 4 == c, d == 0))
        def _():
            for k in range(2):
                for p in (1, 0):
                    done(c2p.at[k, p], s_c2p.at[k, p])
                    done(c2m.at[k, p], s_c2m.at[k, p])
                    total = quarter(b4, sides[k], p)[...].astype(F32) + c2p[k, p].astype(F32) + c2m[k, p].astype(F32)
                    if k == 0:
                        zs[p] = total.astype(BF16)
                        send(zs.at[p], zr.at[p], t_c, s_z.at[p], zo)
                    else:
                        own[p] = total

    block_step(0)

    def forward(e_x, hh, e):
        left, right = lax.rem(x + 3, 4), lax.rem(x + 1, 4)
        done(rows(H, hrow(c, left, hh), 64), s_bxp.at[e, 0])
        share(left, hh, 0, xp, s_bfp.at[e])
        done(rows(H, hrow(c, right, hh) + 64, 64), s_bxm.at[e, 1])
        share(right, hh, 1, xm, s_bfm.at[e])

    def across_near(hh, e):
        left, right = lax.rem(x + 3, 4), lax.rem(x + 1, 4)
        done(rows(H, hrow(c, left, hh) + 64, 64), s_bxp.at[e, 1])
        hid_across(left, hh)
        done(rows(H, hrow(c, right, hh), 64), s_bxm.at[e, 0])
        hid_across(right, hh)

    def across_far(hh, e):
        far = lax.rem(x + 2, 4)
        done(rows(H, hrow(c, far, hh), 64), s_bfp.at[e])
        done(rows(H, hrow(c, far, hh) + 64, 64), s_bfm.at[e])
        hid_across(far, hh)

    def from_z(part):
        done(rows(H, hrow(c, x, 1 - h) + part * 64, 64), s_bz.at[part])
        first, second = (xp, xm) if part == 0 else (xm, xp)
        share(x, 1 - h, part, xp, s_bxp.at[1, part])
        share(x, 1 - h, part, xm, s_bxm.at[1, part])
        if part == 1:
            hid_across(x, 1 - h)

    tasks = {
        (1, 0): [lambda: forward(x, h, 0)],
        (1, 2): [lambda: from_z(0), lambda: add_step(0)],
        (2, 0): [lambda: from_z(1), lambda: sum_step(0)],
        (2, 1): [lambda: across_near(h, 0)],
        (2, 2): [lambda: add_step(1), lambda: add_step(-1)],
        (2, 3): [lambda: across_far(h, 0)],
        (3, 0): [lambda: sum_step(1), lambda: sum_step(-1)],
        (3, 1): [lambda: forward(x, 1 - h, 1)],
        (3, 2): [lambda: add_step(2), lambda: add_step(-2), lambda: across_near(1 - h, 1)],
        (4, 0): [lambda: sum_step(2), lambda: sum_step(-2)],
        (4, 1): [],
    }
    for stage in range(1, 5):
        plus = lax.rem(y - stage + 8, 8)
        minus = lax.rem(y + stage, 8)
        for i in range(4 if stage < 4 else 2):
            n = (stage - 1) * 4 + i
            ip, im = (i, i) if stage < 4 else (i, i + 2)
            piece = rows(U, urow(plus, ip), 64)
            done(piece, s_yp.at[n])
            if n < 10:
                send(piece, piece, t_u, s_yp.at[n + 4], yp)
            to_partner(plus, ip)
            piece = rows(U, urow(minus, im), 64)
            done(piece, s_ym.at[n])
            if n < 8:
                send(piece, piece, t_u, s_ym.at[n + 4], ym)
            elif n in (10, 11):
                send(piece, piece, t_u, s_ym.at[n + 2], ym)
            to_partner(minus, im)
            for task in tasks.get((stage, i), []):
                task()
        if stage < 4:
            block_step(-stage)
            block_step(stage)
        else:
            block_step(4)

    across_far(1 - h, 1)
    add_step(3)
    add_step(-3)
    done(rows(H, (1 - c) * 1024, 1024), s_hd.at[0])

    def dw_tile(f):
        cols = slice(f * 128, f * 128 + 128)
        dwv[cols] = lax.dot_general(H[:, cols], U[...], (((0,), (0,)), ((), ())), preferred_element_type=F32)
        pltpu.make_async_copy(dwv.at[cols], dw_out.at[cols], t_out).start()

    dw_tile(0)
    add_step(4)
    dw_tile(1)
    sum_step(3)
    sum_step(-3)
    dw_tile(2)
    dw_tile(3)
    sum_step(4)
    dw_tile(4)
    dw_tile(5)
    dw_tile(6)
    for p in range(2):
        done(zr.at[p], s_z.at[p])
        igv[p] = (own[p] + zr[p].astype(F32)).astype(BF16)
        pltpu.make_async_copy(igv.at[p], ig_out.at[p * 64 : p * 64 + 64], s_loc.at[p]).start()

    done(rows(U, 0, 1984), t_u)
    done(UP, t_up)
    done(W, t_w)
    done(rows(H, 0, 1024), t_hd)
    done(rows(H, 0, 896), t_h)
    done(rows(H, 0, 896), t_c)
    done(dwv, t_out)
    done(igv.at[0], s_loc.at[0])
    done(igv.at[1], s_loc.at[1])


def local(hidden, upstream, weight):
    dma = pltpu.SemaphoreType.DMA
    return pl.pallas_call(
        kernel,
        out_shape=(jax.ShapeDtypeStruct((128, 896), BF16), jax.ShapeDtypeStruct((896, 512), F32)),
        in_specs=[pl.BlockSpec(memory_space=pl.ANY)] * 3,
        out_specs=[pl.BlockSpec(memory_space=pl.ANY)] * 2,
        scratch_shapes=[
            pltpu.VMEM((2048, 512), BF16),
            pltpu.VMEM((1024, 512), BF16),
            pltpu.VMEM((2048, 896), BF16),
            pltpu.VMEM((896, 512), BF16),
            pltpu.VMEM((896, 512), BF16),
            pltpu.VMEM((4, 256, 896), BF16),
            pltpu.VMEM((2, 64, 896), BF16),
            pltpu.VMEM((2, 64, 896), BF16),
            pltpu.VMEM((2, 2, 64, 896), BF16),
            pltpu.VMEM((2, 2, 64, 896), BF16),
            pltpu.VMEM((2, 64, 896), BF16),
            pltpu.VMEM((2, 64, 896), BF16),
            pltpu.VMEM((2, 64, 896), F32),
            pltpu.VMEM((2, 64, 896), BF16),
            pltpu.VMEM((896, 512), F32),
            dma((3,)), dma((3,)), dma((14,)), dma((14,)), dma((4,)), dma((1,)), dma((2,)),
            dma((2, 2)), dma((2, 2)), dma((2,)), dma((2,)), dma((1,)),
            dma((2,)), dma((2,)), dma((2, 2)), dma((2, 2)), dma((2,)),
            dma, dma, dma, dma, dma, dma, dma,
        ],
        compiler_params=pltpu.CompilerParams(
            collective_id=0, has_side_effects=True, vmem_limit_bytes=48 << 20
        ),
    )(hidden, upstream, weight)


def solution(mesh):
    finer = Mesh(mesh.devices.reshape(2, 4, 2, 8, 4), ("dp", "x", "zh", "y", "zl"))
    placed = (P(DP_ROW, COL), P(COL, DP_ROW), P(COL, DP_ROW))
    return jax.shard_map(
        local,
        mesh=finer,
        in_specs=placed,
        out_specs=(P(DP_ROW, COL), P(COL, DP_ROW)),
        check_vma=False,
    )
```

```python
import jax
import jax.numpy as jnp
from jax import lax
from jax.experimental import pallas as pl
from jax.experimental.pallas import tpu as pltpu
from jax.sharding import Mesh
from jax.sharding import PartitionSpec as P

DP_ROW = ("dp", "x", "zh")
COL = ("y", "zl")
MESH = pl.DeviceIdType.MESH
BF16 = jnp.bfloat16
F32 = jnp.float32


def rows(ref, start, count):
    return ref.at[pl.ds(pl.multiple_of(start, 64), count)]


def done(ref, sem):
    pltpu.make_async_copy(ref, ref, sem).wait()


STEPS = (
    "01", "10", "02", "11", "03", "bz:0", "wp:0", "fwd:0",
    "20", "T:0", "bz:1", "12", "13", "21", "T:1", "T:-1",
    "far:0", "fz:0", "fz:1", "22", "near:0", "23", "add:0", "adb:0",
    "30", "T:2", "T:-2", "31", "add:1", "add:-1", "adb:1", "adb:-1",
    "32", "sum:0", "33", "40", "T:-3", "T:3", "41", "42",
    "add:-2", "add:2", "adb:-2", "adb:2", "43",
)
TAIL = (
    "T:4", "z:0", "z:1", "sum:1", "sum:-1", "sum:-2", "sum:2", "add:-3",
    "add:3", "adb:-3", "adb:3", "add:4", "adb:4", "near:1", "far:1", "hd:0",
    "dw:0", "sum:-3", "sum:3", "dw:1", "sum:4", "own:0", "own:1", "own:-1",
    "own:2", "own:-2", "own:-3", "own:3", "own:4", "dw:2", "dw:3", "dw:4",
    "dw:5", "dw:6",
)


def kernel(
    hid_in, up_in, w_in, ig_out, dw_out,
    U, UP, H, W, WP, T, c1p, c1m, c2p, c2m, zs, zr, own,
    s_loc, s_a1, s_yp, s_ym, s_up, s_w, s_bz, s_bxp, s_bxm, s_bf, s_bfz, s_hd,
    s_c1p, s_c1m, s_c2p, s_c2m, s_z,
    t_u, t_up, t_w, t_h, t_hd, t_c,
):
    c = lax.axis_index("dp")
    x = lax.axis_index("x")
    h = lax.axis_index("zh")
    y = lax.axis_index("y")
    l = lax.axis_index("zl")
    other = {"dp": 1 - c}
    xp = {"x": lax.rem(x + 1, 4)}
    xm = {"x": lax.rem(x + 3, 4)}
    yp = {"y": lax.rem(y + 1, 8)}
    ym = {"y": lax.rem(y + 7, 8)}
    zo = {"zh": 1 - h}
    line = [l, l + 1 - 2 * lax.rem(l, 2), lax.rem(l + 2, 4), 3 - l]
    mates = [{"zl": k} for k in line[1:]]

    def send(src, dst, t, s, to):
        pltpu.make_async_remote_copy(
            src_ref=src, dst_ref=dst, send_sem=t, recv_sem=s, device_id=to, device_id_type=MESH
        ).start()

    def urow(block, i):
        return (block * 4 + line[i]) * 64

    def hrow(core, xx, hh):
        return (core * 8 + xx * 2 + hh) * 128

    local_up = pltpu.make_async_copy(up_in, rows(U, urow(y, 0), 64), s_loc.at[0])
    local_hid = pltpu.make_async_copy(hid_in, rows(H, hrow(c, x, h), 128), s_loc.at[1])
    local_w = pltpu.make_async_copy(w_in, W, s_loc.at[2])
    local_up.start()
    local_hid.start()
    local_w.start()

    barrier = pltpu.get_barrier_semaphore()
    partners = mates + [yp, ym, xp, xm, zo, other]
    for to in partners:
        pl.semaphore_signal(barrier, inc=1, device_id=to, device_id_type=MESH)
    with jax.named_scope('barrier'):
        pl.semaphore_wait(barrier, len(partners))

    with jax.named_scope('lup'):
        local_up.wait()
    mine = rows(U, urow(y, 0), 64)
    for i in range(1, 4):
        send(mine, mine, t_u, s_a1.at[i - 1], mates[i - 1])

    def to_partner(block, i):
        @pl.when(block // 4 != c)
        def _():
            b4 = lax.rem(block, 4)
            send(rows(U, urow(block, i), 64), rows(UP, (b4 * 4 + line[i]) * 64, 64), t_up, s_up.at[b4], other)

    to_partner(y, 0)
    send(mine, mine, t_u, s_yp.at[0], yp)
    send(mine, mine, t_u, s_ym.at[0], ym)

    with jax.named_scope('lhid'):
        local_hid.wait()

    def share(xx, hh, part, to, sem):
        piece = rows(H, hrow(c, xx, hh) + part * 64, 64)
        send(piece, piece, t_h, sem, to)

    share(x, h, 0, xp, s_bxp.at[0, 0])
    share(x, h, 1, xm, s_bxm.at[0, 1])
    share(x, h, 1, xp, s_bxp.at[0, 1])
    share(x, h, 0, xm, s_bxm.at[0, 0])

    def hid_across(xx, hh):
        piece = rows(H, hrow(c, xx, hh), 128)
        send(piece, piece, t_hd, s_hd.at[0], other)

    hid_across(x, h)
    with jax.named_scope('lw'):
        local_w.wait()
    send(W, WP, t_w, s_w.at[0], other)

    wp = rows(WP, 0, 896)

    def quarter(xx, hh, ab):
        return T.at[xx, pl.ds(pl.multiple_of(hh * 128 + ab * 64, 64), 64)]

    sides = (1 - h, h)

    def place_of(delta):
        block = lax.rem(y + delta + 8, 8)
        b4 = lax.rem(block, 4)
        return block, b4, block // 4 == c, lax.rem(b4 - x + 4, 4)

    def spread(delta):
        _, b4, here, d = place_of(delta)

        @pl.when(jnp.logical_and(here, d == 2))
        def _():
            for k in range(2):
                send(quarter(b4, sides[k], 0), c1p.at[k], t_c, s_c1p.at[k], xp)
                send(quarter(b4, sides[k], 1), c1m.at[k], t_c, s_c1m.at[k], xm)

        @pl.when(jnp.logical_and(here, d == 1))
        def _():
            for k in range(2):
                send(quarter(b4, sides[k], 1), c2p.at[k, 1], t_c, s_c2p.at[k, 1], xp)

        @pl.when(jnp.logical_and(here, d == 3))
        def _():
            for k in range(2):
                send(quarter(b4, sides[k], 0), c2m.at[k, 0], t_c, s_c2m.at[k, 0], xm)

    def block_step(delta):
        block, b4, here, d = place_of(delta)

        @pl.when(here)
        def _():
            done(rows(UP, b4 * 256, 256), s_up.at[b4])
            u = rows(U, block * 256, 256)
            up = rows(UP, b4 * 256, 256)
            dims = (((1,), (1,)), ((), ()))
            for n0 in range(0, 896, 256):
                n1 = min(n0 + 256, 896)
                acc = lax.dot_general(u[...], W[n0:n1], dims, preferred_element_type=F32)
                acc += lax.dot_general(up[...], WP[n0:n1], dims, preferred_element_type=F32)
                T[b4, :, n0:n1] = acc.astype(BF16)

        spread(delta)

    def add_step(delta, k):
        _, b4, here, d = place_of(delta)

        @pl.when(jnp.logical_and(here, d == 1))
        def _():
            done(c1p.at[k], s_c1p.at[k])
            q = quarter(b4, sides[k], 0)
            q[...] = (q[...].astype(F32) + c1p[k].astype(F32)).astype(BF16)
            send(q, c2p.at[k, 0], t_c, s_c2p.at[k, 0], xp)

        @pl.when(jnp.logical_and(here, d == 3))
        def _():
            done(c1m.at[k], s_c1m.at[k])
            q = quarter(b4, sides[k], 1)
            q[...] = (q[...].astype(F32) + c1m[k].astype(F32)).astype(BF16)
            send(q, c2m.at[k, 1], t_c, s_c2m.at[k, 1], xm)

    def sum_step(delta, k):
        _, b4, here, d = place_of(delta)

        @pl.when(jnp.logical_and(here, d == 0))
        def _():
            for p in (1, 0):
                done(c2p.at[k, p], s_c2p.at[k, p])
                done(c2m.at[k, p], s_c2m.at[k, p])
                total = quarter(b4, sides[k], p)[...].astype(F32) + c2p[k, p].astype(F32) + c2m[k, p].astype(F32)
                if k == 0:
                    zs[p] = total.astype(BF16)
                    send(zs.at[p], zr.at[p], t_c, s_z.at[p], zo)
                else:
                    own[p] = total

    def last_step():
        for p in range(2):
            done(zr.at[p], s_z.at[p])
            ig_out[p * 64 : p * 64 + 64] = (own[p] + zr[p].astype(F32)).astype(BF16)

    def forward(hh, e):
        left, right = lax.rem(x + 3, 4), lax.rem(x + 1, 4)
        done(rows(H, hrow(c, left, hh), 64), s_bxp.at[e, 0])
        share(left, hh, 0, xp, s_bf.at[0])
        done(rows(H, hrow(c, right, hh) + 64, 64), s_bxm.at[e, 1])
        share(right, hh, 1, xm, s_bf.at[1])

    def across_near(hh, e):
        left, right = lax.rem(x + 3, 4), lax.rem(x + 1, 4)
        for part in (0, 1) if e == 1 else (1,):
            done(rows(H, hrow(c, left, hh) + part * 64, 64), s_bxp.at[e, part])
        hid_across(left, hh)
        for part in (1, 0) if e == 1 else (0,):
            done(rows(H, hrow(c, right, hh) + part * 64, 64), s_bxm.at[e, part])
        hid_across(right, hh)

    def across_far(hh, e):
        far = lax.rem(x + 2, 4)
        s_a, s_b = (s_bf.at[0], s_bf.at[1]) if e == 0 else (s_bfz.at[0], s_bfz.at[1])
        done(rows(H, hrow(c, far, hh), 64), s_a)
        done(rows(H, hrow(c, far, hh) + 64, 64), s_b)
        hid_across(far, hh)

    def far_along_z(part):
        share(lax.rem(x + 2, 4), h, part, zo, s_bfz.at[part])

    def from_z(part):
        done(rows(H, hrow(c, x, 1 - h) + part * 64, 64), s_bz.at[part])
        first, second = (xp, xm) if part == 0 else (xm, xp)
        share(x, 1 - h, part, xp, s_bxp.at[1, part])
        share(x, 1 - h, part, xm, s_bxm.at[1, part])
        if part == 1:
            hid_across(x, 1 - h)

    def halves():
        done(rows(H, (1 - c) * 1024, 1024), s_hd.at[0])

    def dw_tile(f):
        cols = slice(f * 128, f * 128 + 128)
        dw_out[cols] = lax.dot_general(H[:, cols], U[...], (((0,), (0,)), ((), ())), preferred_element_type=F32)

    ways = {
        "T": block_step,
        "add": lambda delta: add_step(delta, 0),
        "adb": lambda delta: add_step(delta, 1),
        "sum": lambda delta: sum_step(delta, 0),
        "own": lambda delta: sum_step(delta, 1),
        "dw": dw_tile,
        "z": from_z,
        "bz": lambda p: share(x, h, p, zo, s_bz.at[p]),
        "fwd": lambda _: forward(h, 0),
        "fz": far_along_z,
        "near": lambda e: across_near((h, 1 - h)[e], e),
        "far": lambda e: across_far((h, 1 - h)[e], e),
        "hd": lambda _: halves(),
        "wp": lambda _: done(wp, s_w.at[0]),
    }

    def run(line_of_tasks):
        for task in line_of_tasks:
            name, number = task.split(":")
            with jax.named_scope(task.replace(":", "_").replace("-", "m")):
                ways[name](int(number))

    def onward(k, i):
        if k == 0:
            piece = rows(U, urow(y, i), 64)
            with jax.named_scope(f"a1_{i}"):
                done(piece, s_a1.at[i - 1])
            send(piece, piece, t_u, s_yp.at[i], yp)
            send(piece, piece, t_u, s_ym.at[i], ym)
            to_partner(y, i)
            return
        n = k * 4 + i
        for block, sem, to, last in (
            (lax.rem(y - k + 8, 8), s_yp, yp, (0, 1)),
            (lax.rem(y + k, 8), s_ym, ym, (2, 3)),
        ):
            if k == 4 and i not in last:
                continue
            piece = rows(U, urow(block, i), 64)
            with jax.named_scope(f"y{k}_{i}"):
                done(piece, sem.at[n - 4])
            if k < 3 or (k == 3 and i in last):
                send(piece, piece, t_u, sem.at[n], to)
            to_partner(block, i)

    for step in STEPS:
        if ":" in step:
            run((step,))
        else:
            onward(int(step[0]), int(step[1]))
    run(TAIL)
    with jax.named_scope('last'):
        last_step()

    with jax.named_scope('fin'):
        done(rows(U, 0, 1984), t_u)
    done(UP, t_up)
    done(W, t_w)
    done(rows(H, 0, 1024), t_hd)
    done(rows(H, 0, 896), t_h)
    done(rows(H, 0, 896), t_c)


def local(hidden, upstream, weight):
    dma = pltpu.SemaphoreType.DMA
    hidden, upstream, weight = (pltpu.with_memory_space_constraint(a, pltpu.HBM) for a in (hidden, upstream, weight))
    return pl.pallas_call(
        kernel,
        out_shape=(jax.ShapeDtypeStruct((128, 896), BF16), jax.ShapeDtypeStruct((896, 512), F32)),
        in_specs=[pl.BlockSpec(memory_space=pltpu.HBM)] * 3,
        out_specs=[pl.BlockSpec(memory_space=pltpu.VMEM)] * 2,
        scratch_shapes=[
            pltpu.VMEM((2048, 512), BF16),
            pltpu.VMEM((1024, 512), BF16),
            pltpu.VMEM((2048, 896), BF16),
            pltpu.VMEM((896, 512), BF16),
            pltpu.VMEM((896, 512), BF16),
            pltpu.VMEM((4, 256, 896), BF16),
            pltpu.VMEM((2, 64, 896), BF16),
            pltpu.VMEM((2, 64, 896), BF16),
            pltpu.VMEM((2, 2, 64, 896), BF16),
            pltpu.VMEM((2, 2, 64, 896), BF16),
            pltpu.VMEM((2, 64, 896), BF16),
            pltpu.VMEM((2, 64, 896), BF16),
            pltpu.VMEM((2, 64, 896), F32),
            dma((3,)), dma((3,)), dma((16,)), dma((16,)), dma((4,)), dma((1,)), dma((2,)),
            dma((2, 2)), dma((2, 2)), dma((2,)), dma((2,)), dma((1,)),
            dma((2,)), dma((2,)), dma((2, 2)), dma((2, 2)), dma((2,)),
            dma, dma, dma, dma, dma, dma,
        ],
        compiler_params=pltpu.CompilerParams(
            collective_id=0, has_side_effects=True, vmem_limit_bytes=40 << 20
        ),
    )(hidden, upstream, weight)


def solution(mesh):
    finer = Mesh(mesh.devices.reshape(2, 4, 2, 8, 4), ("dp", "x", "zh", "y", "zl"))
    placed = (P(DP_ROW, COL), P(COL, DP_ROW), P(COL, DP_ROW))
    return jax.shard_map(
        local,
        mesh=finer,
        in_specs=placed,
        out_specs=(P(DP_ROW, COL), P(COL, DP_ROW)),
        check_vma=False,
    )
```

```python
import jax
import jax.numpy as jnp
from jax import lax
from jax.experimental import pallas as pl
from jax.experimental.pallas import tpu as pltpu
from jax.sharding import Mesh
from jax.sharding import PartitionSpec as P

DP_ROW = ("dp", "x", "zh")
COL = ("y", "zl")
MESH = pl.DeviceIdType.MESH
BF16 = jnp.bfloat16
F32 = jnp.float32


def rows(ref, start, count):
    return ref.at[pl.ds(pl.multiple_of(start, 64), count)]


def done(ref, sem):
    pltpu.make_async_copy(ref, ref, sem).wait()


STEPS = (
    "10", "01", "02", "20", "03", "bz:0", "wp:0", "fwd:0",
    "11", "T:0", "bz:1", "12", "13", "21", "T:1", "T:-1",
    "far:0", "fz:0", "fz:1", "22", "near:0", "23", "add:0", "adb:0",
    "30", "T:2", "T:-2", "31", "add:1", "add:-1", "adb:1", "adb:-1",
    "32", "sum:0", "33", "40", "T:-3", "T:3", "41", "42",
    "add:-2", "add:2", "adb:-2", "adb:2", "43", "T:4",
)
TAIL = (
    "z:0", "z:1", "sum:1", "sum:-1", "add:-3", "add:3", "adb:-3", "adb:3",
    "sum:-2", "sum:2", "add:4", "adb:4", "sum:-3", "sum:3", "near:1", "sum:4",
    "far:1", "hd:0", "dw:0", "dw:1", "dw:2", "own:0", "own:1", "own:-1",
    "own:2", "own:-2", "own:-3", "own:3", "own:4", "dw:3", "dw:4", "dw:5",
    "dw:6",
)


def kernel(
    hid_in, up_in, w_in, ig_out, dw_out,
    U, UP, H, W, WP, T, c1p, c1m, c2p, c2m, zs, zr, own,
    s_loc, s_a1, s_yp, s_ym, s_up, s_w, s_bz, s_bxp, s_bxm, s_bf, s_bfz, s_hd,
    s_c1p, s_c1m, s_c2p, s_c2m, s_z,
    t_u, t_up, t_w, t_h, t_hd, t_c,
):
    c = lax.axis_index("dp")
    x = lax.axis_index("x")
    h = lax.axis_index("zh")
    y = lax.axis_index("y")
    l = lax.axis_index("zl")
    other = {"dp": 1 - c}
    xp = {"x": lax.rem(x + 1, 4)}
    xm = {"x": lax.rem(x + 3, 4)}
    yp = {"y": lax.rem(y + 1, 8)}
    ym = {"y": lax.rem(y + 7, 8)}
    zo = {"zh": 1 - h}
    line = [l, l + 1 - 2 * lax.rem(l, 2), lax.rem(l + 2, 4), 3 - l]
    mates = [{"zl": k} for k in line[1:]]

    def send(src, dst, t, s, to):
        pltpu.make_async_remote_copy(
            src_ref=src, dst_ref=dst, send_sem=t, recv_sem=s, device_id=to, device_id_type=MESH
        ).start()

    def urow(block, i):
        return (block * 4 + line[i]) * 64

    def hrow(core, xx, hh):
        return (core * 8 + xx * 2 + hh) * 128

    local_up = pltpu.make_async_copy(up_in, rows(U, urow(y, 0), 64), s_loc.at[0])
    local_hid = pltpu.make_async_copy(hid_in, rows(H, hrow(c, x, h), 128), s_loc.at[1])
    local_w = pltpu.make_async_copy(w_in, W, s_loc.at[2])
    local_up.start()
    local_hid.start()
    local_w.start()

    barrier = pltpu.get_barrier_semaphore()
    partners = mates + [yp, ym, xp, xm, zo, other]
    for to in partners:
        pl.semaphore_signal(barrier, inc=1, device_id=to, device_id_type=MESH)
    with jax.named_scope('barrier'):
        pl.semaphore_wait(barrier, len(partners))

    with jax.named_scope('lup'):
        local_up.wait()
    mine = rows(U, urow(y, 0), 64)
    for i in range(1, 4):
        send(mine, mine, t_u, s_a1.at[i - 1], mates[i - 1])

    def to_partner(block, i):
        @pl.when(block // 4 != c)
        def _():
            b4 = lax.rem(block, 4)
            send(rows(U, urow(block, i), 64), rows(UP, (b4 * 4 + line[i]) * 64, 64), t_up, s_up.at[b4], other)

    to_partner(y, 0)
    send(mine, mine, t_u, s_yp.at[0], yp)
    send(mine, mine, t_u, s_ym.at[0], ym)

    with jax.named_scope('lhid'):
        local_hid.wait()

    def share(xx, hh, part, to, sem):
        piece = rows(H, hrow(c, xx, hh) + part * 64, 64)
        send(piece, piece, t_h, sem, to)

    share(x, h, 0, xp, s_bxp.at[0, 0])
    share(x, h, 1, xm, s_bxm.at[0, 1])
    share(x, h, 1, xp, s_bxp.at[0, 1])
    share(x, h, 0, xm, s_bxm.at[0, 0])

    def hid_across(xx, hh):
        piece = rows(H, hrow(c, xx, hh), 128)
        send(piece, piece, t_hd, s_hd.at[0], other)

    hid_across(x, h)
    with jax.named_scope('lw'):
        local_w.wait()
    send(W, WP, t_w, s_w.at[0], other)

    wp = rows(WP, 0, 896)

    def quarter(xx, hh, ab):
        return T.at[xx, pl.ds(pl.multiple_of(hh * 128 + ab * 64, 64), 64)]

    sides = (1 - h, h)

    def place_of(delta):
        block = lax.rem(y + delta + 8, 8)
        b4 = lax.rem(block, 4)
        return block, b4, block // 4 == c, lax.rem(b4 - x + 4, 4)

    def spread(delta):
        _, b4, here, d = place_of(delta)

        @pl.when(jnp.logical_and(here, d == 2))
        def _():
            for k in range(2):
                send(quarter(b4, sides[k], 0), c1p.at[k], t_c, s_c1p.at[k], xp)
                send(quarter(b4, sides[k], 1), c1m.at[k], t_c, s_c1m.at[k], xm)

        @pl.when(jnp.logical_and(here, d == 1))
        def _():
            for k in range(2):
                send(quarter(b4, sides[k], 1), c2p.at[k, 1], t_c, s_c2p.at[k, 1], xp)

        @pl.when(jnp.logical_and(here, d == 3))
        def _():
            for k in range(2):
                send(quarter(b4, sides[k], 0), c2m.at[k, 0], t_c, s_c2m.at[k, 0], xm)

    def block_step(delta):
        block, b4, here, d = place_of(delta)

        @pl.when(here)
        def _():
            done(rows(UP, b4 * 256, 256), s_up.at[b4])
            u = rows(U, block * 256, 256)
            up = rows(UP, b4 * 256, 256)
            dims = (((1,), (1,)), ((), ()))
            for n0 in range(0, 896, 256):
                n1 = min(n0 + 256, 896)
                acc = lax.dot_general(u[...], W[n0:n1], dims, preferred_element_type=F32)
                acc += lax.dot_general(up[...], WP[n0:n1], dims, preferred_element_type=F32)
                T[b4, :, n0:n1] = acc.astype(BF16)

        spread(delta)

    def add_step(delta, k):
        _, b4, here, d = place_of(delta)

        @pl.when(jnp.logical_and(here, d == 1))
        def _():
            done(c1p.at[k], s_c1p.at[k])
            q = quarter(b4, sides[k], 0)
            q[...] = (q[...].astype(F32) + c1p[k].astype(F32)).astype(BF16)
            send(q, c2p.at[k, 0], t_c, s_c2p.at[k, 0], xp)

        @pl.when(jnp.logical_and(here, d == 3))
        def _():
            done(c1m.at[k], s_c1m.at[k])
            q = quarter(b4, sides[k], 1)
            q[...] = (q[...].astype(F32) + c1m[k].astype(F32)).astype(BF16)
            send(q, c2m.at[k, 1], t_c, s_c2m.at[k, 1], xm)

    def sum_step(delta, k):
        _, b4, here, d = place_of(delta)

        @pl.when(jnp.logical_and(here, d == 0))
        def _():
            for p in (1, 0):
                done(c2p.at[k, p], s_c2p.at[k, p])
                done(c2m.at[k, p], s_c2m.at[k, p])
                total = quarter(b4, sides[k], p)[...].astype(F32) + c2p[k, p].astype(F32) + c2m[k, p].astype(F32)
                if k == 0:
                    zs[p] = total.astype(BF16)
                    send(zs.at[p], zr.at[p], t_c, s_z.at[p], zo)
                else:
                    own[p] = total

    def last_step():
        for p in range(2):
            done(zr.at[p], s_z.at[p])
            ig_out[p * 64 : p * 64 + 64] = (own[p] + zr[p].astype(F32)).astype(BF16)

    def forward(hh, e):
        left, right = lax.rem(x + 3, 4), lax.rem(x + 1, 4)
        done(rows(H, hrow(c, left, hh), 64), s_bxp.at[e, 0])
        share(left, hh, 0, xp, s_bf.at[0])
        done(rows(H, hrow(c, right, hh) + 64, 64), s_bxm.at[e, 1])
        share(right, hh, 1, xm, s_bf.at[1])

    def across_near(hh, e):
        left, right = lax.rem(x + 3, 4), lax.rem(x + 1, 4)
        for part in (0, 1) if e == 1 else (1,):
            done(rows(H, hrow(c, left, hh) + part * 64, 64), s_bxp.at[e, part])
        hid_across(left, hh)
        for part in (1, 0) if e == 1 else (0,):
            done(rows(H, hrow(c, right, hh) + part * 64, 64), s_bxm.at[e, part])
        hid_across(right, hh)

    def across_far(hh, e):
        far = lax.rem(x + 2, 4)
        s_a, s_b = (s_bf.at[0], s_bf.at[1]) if e == 0 else (s_bfz.at[0], s_bfz.at[1])
        done(rows(H, hrow(c, far, hh), 64), s_a)
        done(rows(H, hrow(c, far, hh) + 64, 64), s_b)
        hid_across(far, hh)

    def far_along_z(part):
        share(lax.rem(x + 2, 4), h, part, zo, s_bfz.at[part])

    def from_z(part):
        done(rows(H, hrow(c, x, 1 - h) + part * 64, 64), s_bz.at[part])
        first, second = (xp, xm) if part == 0 else (xm, xp)
        share(x, 1 - h, part, xp, s_bxp.at[1, part])
        share(x, 1 - h, part, xm, s_bxm.at[1, part])
        if part == 1:
            hid_across(x, 1 - h)

    def halves():
        done(rows(H, (1 - c) * 1024, 1024), s_hd.at[0])

    def dw_tile(f):
        cols = slice(f * 128, f * 128 + 128)
        dw_out[cols] = lax.dot_general(H[:, cols], U[...], (((0,), (0,)), ((), ())), preferred_element_type=F32)

    ways = {
        "T": block_step,
        "add": lambda delta: add_step(delta, 0),
        "adb": lambda delta: add_step(delta, 1),
        "sum": lambda delta: sum_step(delta, 0),
        "own": lambda delta: sum_step(delta, 1),
        "dw": dw_tile,
        "z": from_z,
        "bz": lambda p: share(x, h, p, zo, s_bz.at[p]),
        "fwd": lambda _: forward(h, 0),
        "fz": far_along_z,
        "near": lambda e: across_near((h, 1 - h)[e], e),
        "far": lambda e: across_far((h, 1 - h)[e], e),
        "hd": lambda _: halves(),
        "wp": lambda _: done(wp, s_w.at[0]),
    }

    def run(line_of_tasks):
        for task in line_of_tasks:
            name, number = task.split(":")
            with jax.named_scope(task.replace(":", "_").replace("-", "m")):
                ways[name](int(number))

    def onward(k, i):
        if k == 0:
            piece = rows(U, urow(y, i), 64)
            with jax.named_scope(f"a1_{i}"):
                done(piece, s_a1.at[i - 1])
            send(piece, piece, t_u, s_yp.at[i], yp)
            send(piece, piece, t_u, s_ym.at[i], ym)
            to_partner(y, i)
            return
        n = k * 4 + i
        for block, sem, to, last in (
            (lax.rem(y - k + 8, 8), s_yp, yp, (0, 1)),
            (lax.rem(y + k, 8), s_ym, ym, (2, 3)),
        ):
            if k == 4 and i not in last:
                continue
            piece = rows(U, urow(block, i), 64)
            with jax.named_scope(f"y{k}_{i}"):
                done(piece, sem.at[n - 4])
            if k < 3 or (k == 3 and i in last):
                send(piece, piece, t_u, sem.at[n], to)
            to_partner(block, i)

    for step in STEPS:
        if ":" in step:
            run((step,))
        else:
            onward(int(step[0]), int(step[1]))
    run(TAIL)
    with jax.named_scope('last'):
        last_step()

    with jax.named_scope('fin'):
        done(rows(U, 0, 1984), t_u)
    done(UP, t_up)
    done(W, t_w)
    done(rows(H, 0, 1024), t_hd)
    done(rows(H, 0, 896), t_h)
    done(rows(H, 0, 896), t_c)


def local(hidden, upstream, weight):
    dma = pltpu.SemaphoreType.DMA
    hidden, upstream, weight = (pltpu.with_memory_space_constraint(a, pltpu.HBM) for a in (hidden, upstream, weight))
    return pl.pallas_call(
        kernel,
        out_shape=(jax.ShapeDtypeStruct((128, 896), BF16), jax.ShapeDtypeStruct((896, 512), F32)),
        in_specs=[pl.BlockSpec(memory_space=pltpu.HBM)] * 3,
        out_specs=[pl.BlockSpec(memory_space=pltpu.VMEM)] * 2,
        scratch_shapes=[
            pltpu.VMEM((2048, 512), BF16),
            pltpu.VMEM((1024, 512), BF16),
            pltpu.VMEM((2048, 896), BF16),
            pltpu.VMEM((896, 512), BF16),
            pltpu.VMEM((896, 512), BF16),
            pltpu.VMEM((4, 256, 896), BF16),
            pltpu.VMEM((2, 64, 896), BF16),
            pltpu.VMEM((2, 64, 896), BF16),
            pltpu.VMEM((2, 2, 64, 896), BF16),
            pltpu.VMEM((2, 2, 64, 896), BF16),
            pltpu.VMEM((2, 64, 896), BF16),
            pltpu.VMEM((2, 64, 896), BF16),
            pltpu.VMEM((2, 64, 896), F32),
            dma((3,)), dma((3,)), dma((16,)), dma((16,)), dma((4,)), dma((1,)), dma((2,)),
            dma((2, 2)), dma((2, 2)), dma((2,)), dma((2,)), dma((1,)),
            dma((2,)), dma((2,)), dma((2, 2)), dma((2, 2)), dma((2,)),
            dma, dma, dma, dma, dma, dma,
        ],
        compiler_params=pltpu.CompilerParams(
            collective_id=0, has_side_effects=True, vmem_limit_bytes=40 << 20
        ),
    )(hidden, upstream, weight)


def solution(mesh):
    finer = Mesh(mesh.devices.reshape(2, 4, 2, 8, 4), ("dp", "x", "zh", "y", "zl"))
    placed = (P(DP_ROW, COL), P(COL, DP_ROW), P(COL, DP_ROW))
    return jax.shard_map(
        local,
        mesh=finer,
        in_specs=placed,
        out_specs=(P(DP_ROW, COL), P(COL, DP_ROW)),
        check_vma=False,
    )
```

```python
import jax
import jax.numpy as jnp
from jax import lax
from jax.experimental import pallas as pl
from jax.experimental.pallas import tpu as pltpu
from jax.sharding import Mesh
from jax.sharding import PartitionSpec as P

DP_ROW = ("dp", "x", "zh")
COL = ("y", "zl")
MESH = pl.DeviceIdType.MESH
BF16 = jnp.bfloat16
F32 = jnp.float32


def rows(ref, start, count):
    return ref.at[pl.ds(pl.multiple_of(start, 64), count)]


def done(ref, sem):
    pltpu.make_async_copy(ref, ref, sem).wait()


STEPS = (
    "10", "01", "02", "20", "03", "bz:0", "wp:0", "fwd:0",
    "11", "T:0", "bz:1", "12", "13", "21", "T:1", "T:-1",
    "far:0", "fz:0", "fz:1", "22", "near:0", "23", "add:0", "adb:0",
    "30", "T:2", "T:-2", "31", "add:1", "add:-1", "adb:1", "adb:-1",
    "32", "sum:0", "33", "40", "T:-3", "T:3", "41", "42",
    "add:-2", "add:2", "adb:-2", "adb:2", "43", "T:4",
)
TAIL = (
    "z:0", "z:1", "sum:1", "sum:-1", "add:-3", "add:3", "adb:-3", "adb:3",
    "sum:-2", "sum:2", "add:4", "adb:4", "sum:-3", "sum:3", "near:1", "sum:4",
    "far:1", "hd:0", "dw:0", "dw:1", "dw:2", "own:0", "own:1", "own:-1",
    "own:2", "own:-2", "own:-3", "own:3", "own:4", "dw:3", "dw:4", "dw:5",
    "dw:6",
)


def kernel(
    hid_in, up_in, w_in, ig_out, dw_out,
    U, UP, H, W, WP, T, c1p, c1m, c2p, c2m, zs, zr, own,
    s_loc, s_a1, s_yp, s_ym, s_up, s_w, s_bz, s_bxp, s_bxm, s_bf, s_bfz, s_hd,
    s_c1p, s_c1m, s_c2p, s_c2m, s_z,
    t_u, t_up, t_w, t_h, t_hd, t_c,
):
    c = lax.axis_index("dp")
    x = lax.axis_index("x")
    h = lax.axis_index("zh")
    y = lax.axis_index("y")
    l = lax.axis_index("zl")
    other = {"dp": 1 - c}
    xp = {"x": lax.rem(x + 1, 4)}
    xm = {"x": lax.rem(x + 3, 4)}
    yp = {"y": lax.rem(y + 1, 8)}
    ym = {"y": lax.rem(y + 7, 8)}
    zo = {"zh": 1 - h}
    line = [l, l + 1 - 2 * lax.rem(l, 2), lax.rem(l + 2, 4), 3 - l]
    mates = [{"zl": k} for k in line[1:]]

    def send(src, dst, t, s, to):
        pltpu.make_async_remote_copy(
            src_ref=src, dst_ref=dst, send_sem=t, recv_sem=s, device_id=to, device_id_type=MESH
        ).start()

    def urow(block, i):
        return (block * 4 + line[i]) * 64

    def hrow(core, xx, hh):
        return (core * 8 + xx * 2 + hh) * 128

    local_up = pltpu.make_async_copy(up_in, rows(U, urow(y, 0), 64), s_loc.at[0])
    local_hid = pltpu.make_async_copy(hid_in, rows(H, hrow(c, x, h), 128), s_loc.at[1])
    local_w = pltpu.make_async_copy(w_in, W, s_loc.at[2])
    local_up.start()
    local_hid.start()
    local_w.start()

    barrier = pltpu.get_barrier_semaphore()
    partners = mates + [yp, ym, xp, xm, zo, other]
    for to in partners:
        pl.semaphore_signal(barrier, inc=1, device_id=to, device_id_type=MESH)
    with jax.named_scope('barrier'):
        pl.semaphore_wait(barrier, len(partners))

    with jax.named_scope('lup'):
        local_up.wait()
    mine = rows(U, urow(y, 0), 64)
    for i in range(1, 4):
        send(mine, mine, t_u, s_a1.at[i - 1], mates[i - 1])

    def to_partner(block, i):
        @pl.when(block // 4 != c)
        def _():
            b4 = lax.rem(block, 4)
            send(rows(U, urow(block, i), 64), rows(UP, (b4 * 4 + line[i]) * 64, 64), t_up, s_up.at[b4], other)

    to_partner(y, 0)
    send(mine, mine, t_u, s_yp.at[0], yp)
    send(mine, mine, t_u, s_ym.at[0], ym)

    with jax.named_scope('lhid'):
        local_hid.wait()

    def share(xx, hh, part, to, sem):
        piece = rows(H, hrow(c, xx, hh) + part * 64, 64)
        send(piece, piece, t_h, sem, to)

    share(x, h, 0, xp, s_bxp.at[0, 0])
    share(x, h, 1, xm, s_bxm.at[0, 1])
    share(x, h, 1, xp, s_bxp.at[0, 1])
    share(x, h, 0, xm, s_bxm.at[0, 0])

    def hid_across(xx, hh):
        piece = rows(H, hrow(c, xx, hh), 128)
        send(piece, piece, t_hd, s_hd.at[0], other)

    hid_across(x, h)
    with jax.named_scope('lw'):
        local_w.wait()
    send(W, WP, t_w, s_w.at[0], other)

    wp = rows(WP, 0, 896)

    def quarter(xx, hh, ab):
        return T.at[xx, pl.ds(pl.multiple_of(hh * 128 + ab * 64, 64), 64)]

    sides = (1 - h, h)

    def place_of(delta):
        block = lax.rem(y + delta + 8, 8)
        b4 = lax.rem(block, 4)
        return block, b4, block // 4 == c, lax.rem(b4 - x + 4, 4)

    def spread(delta):
        _, b4, here, d = place_of(delta)

        @pl.when(jnp.logical_and(here, d == 2))
        def _():
            for k in range(2):
                send(quarter(b4, sides[k], 0), c1p.at[k], t_c, s_c1p.at[k], xp)
                send(quarter(b4, sides[k], 1), c1m.at[k], t_c, s_c1m.at[k], xm)

        @pl.when(jnp.logical_and(here, d == 1))
        def _():
            for k in range(2):
                send(quarter(b4, sides[k], 1), c2p.at[k, 1], t_c, s_c2p.at[k, 1], xp)

        @pl.when(jnp.logical_and(here, d == 3))
        def _():
            for k in range(2):
                send(quarter(b4, sides[k], 0), c2m.at[k, 0], t_c, s_c2m.at[k, 0], xm)

    def block_step(delta):
        block, b4, here, d = place_of(delta)

        @pl.when(here)
        def _():
            done(rows(UP, b4 * 256, 256), s_up.at[b4])
            u = rows(U, block * 256, 256)
            up = rows(UP, b4 * 256, 256)
            dims = (((1,), (1,)), ((), ()))
            for n0 in range(0, 896, 256):
                n1 = min(n0 + 256, 896)
                acc = lax.dot_general(u[...], W[n0:n1], dims, preferred_element_type=F32)
                acc += lax.dot_general(up[...], WP[n0:n1], dims, preferred_element_type=F32)
                T[b4, :, n0:n1] = acc.astype(BF16)

        spread(delta)

    def add_step(delta, k):
        _, b4, here, d = place_of(delta)

        @pl.when(jnp.logical_and(here, d == 1))
        def _():
            done(c1p.at[k], s_c1p.at[k])
            q = quarter(b4, sides[k], 0)
            q[...] = (q[...].astype(F32) + c1p[k].astype(F32)).astype(BF16)
            send(q, c2p.at[k, 0], t_c, s_c2p.at[k, 0], xp)

        @pl.when(jnp.logical_and(here, d == 3))
        def _():
            done(c1m.at[k], s_c1m.at[k])
            q = quarter(b4, sides[k], 1)
            q[...] = (q[...].astype(F32) + c1m[k].astype(F32)).astype(BF16)
            send(q, c2m.at[k, 1], t_c, s_c2m.at[k, 1], xm)

    def sum_step(delta, k):
        _, b4, here, d = place_of(delta)

        @pl.when(jnp.logical_and(here, d == 0))
        def _():
            for p in (1, 0):
                done(c2p.at[k, p], s_c2p.at[k, p])
                done(c2m.at[k, p], s_c2m.at[k, p])
                total = quarter(b4, sides[k], p)[...].astype(F32) + c2p[k, p].astype(F32) + c2m[k, p].astype(F32)
                if k == 0:
                    zs[p] = total.astype(BF16)
                    send(zs.at[p], zr.at[p], t_c, s_z.at[p], zo)
                else:
                    own[p] = total

    def last_step():
        for p in range(2):
            done(zr.at[p], s_z.at[p])
            ig_out[p * 64 : p * 64 + 64] = (own[p] + zr[p].astype(F32)).astype(BF16)

    def forward(hh, e):
        left, right = lax.rem(x + 3, 4), lax.rem(x + 1, 4)
        done(rows(H, hrow(c, left, hh), 64), s_bxp.at[e, 0])
        share(left, hh, 0, xp, s_bf.at[0])
        done(rows(H, hrow(c, right, hh) + 64, 64), s_bxm.at[e, 1])
        share(right, hh, 1, xm, s_bf.at[1])

    def across_near(hh, e):
        left, right = lax.rem(x + 3, 4), lax.rem(x + 1, 4)
        for part in (0, 1) if e == 1 else (1,):
            done(rows(H, hrow(c, left, hh) + part * 64, 64), s_bxp.at[e, part])
        hid_across(left, hh)
        for part in (1, 0) if e == 1 else (0,):
            done(rows(H, hrow(c, right, hh) + part * 64, 64), s_bxm.at[e, part])
        hid_across(right, hh)

    def across_far(hh, e):
        far = lax.rem(x + 2, 4)
        s_a, s_b = (s_bf.at[0], s_bf.at[1]) if e == 0 else (s_bfz.at[0], s_bfz.at[1])
        done(rows(H, hrow(c, far, hh), 64), s_a)
        done(rows(H, hrow(c, far, hh) + 64, 64), s_b)
        hid_across(far, hh)

    def far_along_z(part):
        share(lax.rem(x + 2, 4), h, part, zo, s_bfz.at[part])

    def from_z(part):
        done(rows(H, hrow(c, x, 1 - h) + part * 64, 64), s_bz.at[part])
        first, second = (xp, xm) if part == 0 else (xm, xp)
        share(x, 1 - h, part, xp, s_bxp.at[1, part])
        share(x, 1 - h, part, xm, s_bxm.at[1, part])
        if part == 1:
            hid_across(x, 1 - h)

    def halves():
        done(rows(H, (1 - c) * 1024, 1024), s_hd.at[0])

    def dw_tile(f):
        cols = slice(f * 128, f * 128 + 128)
        dw_out[cols] = lax.dot_general(H[:, cols], U[...], (((0,), (0,)), ((), ())), preferred_element_type=F32)

    ways = {
        "T": block_step,
        "add": lambda delta: add_step(delta, 0),
        "adb": lambda delta: add_step(delta, 1),
        "sum": lambda delta: sum_step(delta, 0),
        "own": lambda delta: sum_step(delta, 1),
        "dw": dw_tile,
        "z": from_z,
        "bz": lambda p: share(x, h, p, zo, s_bz.at[p]),
        "fwd": lambda _: forward(h, 0),
        "fz": far_along_z,
        "near": lambda e: across_near((h, 1 - h)[e], e),
        "far": lambda e: across_far((h, 1 - h)[e], e),
        "hd": lambda _: halves(),
        "wp": lambda _: done(wp, s_w.at[0]),
    }

    def run(line_of_tasks):
        for task in line_of_tasks:
            name, number = task.split(":")
            with jax.named_scope(task.replace(":", "_").replace("-", "m")):
                ways[name](int(number))

    def onward(k, i):
        if k == 0:
            piece = rows(U, urow(y, i), 64)
            with jax.named_scope(f"a1_{i}"):
                done(piece, s_a1.at[i - 1])
            send(piece, piece, t_u, s_yp.at[i], yp)
            send(piece, piece, t_u, s_ym.at[i], ym)
            to_partner(y, i)
            return
        n = k * 4 + i
        for block, sem, to, last in (
            (lax.rem(y - k + 8, 8), s_yp, yp, (0, 1)),
            (lax.rem(y + k, 8), s_ym, ym, (2, 3)),
        ):
            if k == 4 and i not in last:
                continue
            piece = rows(U, urow(block, i), 64)
            with jax.named_scope(f"y{k}_{i}"):
                done(piece, sem.at[n - 4])
            if k < 3 or (k == 3 and i in last):
                send(piece, piece, t_u, sem.at[n], to)
            to_partner(block, i)

    for step in STEPS:
        if ":" in step:
            run((step,))
        else:
            onward(int(step[0]), int(step[1]))
    run(TAIL)
    with jax.named_scope('last'):
        last_step()

    with jax.named_scope('fin'):
        done(rows(U, 0, 1984), t_u)
    done(UP, t_up)
    done(W, t_w)
    done(rows(H, 0, 1024), t_hd)
    done(rows(H, 0, 896), t_h)
    done(rows(H, 0, 896), t_c)


def put_out(grad, weight_grad, grad_out, weight_grad_out, sems):
    copies = [pltpu.make_async_copy(grad, grad_out, sems.at[7])]
    for f in range(7):
        part = pl.ds(f * 128, 128)
        copies.append(pltpu.make_async_copy(weight_grad.at[part], weight_grad_out.at[part], sems.at[f]))
    for copy in copies:
        copy.start()
    for copy in copies:
        copy.wait()


def local(hidden, upstream, weight):
    dma = pltpu.SemaphoreType.DMA
    hidden, upstream, weight = (pltpu.with_memory_space_constraint(a, pltpu.HBM) for a in (hidden, upstream, weight))
    grad, weight_grad = pl.pallas_call(
        kernel,
        out_shape=(jax.ShapeDtypeStruct((128, 896), BF16), jax.ShapeDtypeStruct((896, 512), F32)),
        in_specs=[pl.BlockSpec(memory_space=pltpu.HBM)] * 3,
        out_specs=[pl.BlockSpec(memory_space=pltpu.VMEM)] * 2,
        scratch_shapes=[
            pltpu.VMEM((2048, 512), BF16),
            pltpu.VMEM((1024, 512), BF16),
            pltpu.VMEM((2048, 896), BF16),
            pltpu.VMEM((896, 512), BF16),
            pltpu.VMEM((896, 512), BF16),
            pltpu.VMEM((4, 256, 896), BF16),
            pltpu.VMEM((2, 64, 896), BF16),
            pltpu.VMEM((2, 64, 896), BF16),
            pltpu.VMEM((2, 2, 64, 896), BF16),
            pltpu.VMEM((2, 2, 64, 896), BF16),
            pltpu.VMEM((2, 64, 896), BF16),
            pltpu.VMEM((2, 64, 896), BF16),
            pltpu.VMEM((2, 64, 896), F32),
            dma((3,)), dma((3,)), dma((16,)), dma((16,)), dma((4,)), dma((1,)), dma((2,)),
            dma((2, 2)), dma((2, 2)), dma((2,)), dma((2,)), dma((1,)),
            dma((2,)), dma((2,)), dma((2, 2)), dma((2, 2)), dma((2,)),
            dma, dma, dma, dma, dma, dma,
        ],
        compiler_params=pltpu.CompilerParams(
            collective_id=0, has_side_effects=True, vmem_limit_bytes=40 << 20
        ),
    )(hidden, upstream, weight)
    return pl.pallas_call(
        put_out,
        out_shape=(pltpu.HBM((128, 896), BF16), pltpu.HBM((896, 512), F32)),
        in_specs=[pl.BlockSpec(memory_space=pltpu.VMEM)] * 2,
        out_specs=[pl.BlockSpec(memory_space=pltpu.HBM)] * 2,
        scratch_shapes=[dma((8,))],
        compiler_params=pltpu.CompilerParams(vmem_limit_bytes=8 << 20),
    )(*(pltpu.with_memory_space_constraint(a, pltpu.VMEM) for a in (grad, weight_grad)))


def solution(mesh):
    finer = Mesh(mesh.devices.reshape(2, 4, 2, 8, 4), ("dp", "x", "zh", "y", "zl"))
    placed = (P(DP_ROW, COL), P(COL, DP_ROW), P(COL, DP_ROW))
    return jax.shard_map(
        local,
        mesh=finer,
        in_specs=placed,
        out_specs=(P(DP_ROW, COL), P(COL, DP_ROW)),
        check_vma=False,
    )
```

```python
import jax
import jax.numpy as jnp
from jax import lax
from jax.experimental import pallas as pl
from jax.experimental.pallas import tpu as pltpu
from jax.sharding import Mesh
from jax.sharding import PartitionSpec as P

DP_ROW = ("dp", "x", "zh")
COL = ("y", "zl")
MESH = pl.DeviceIdType.MESH
BF16 = jnp.bfloat16
F32 = jnp.float32


def rows(ref, start, count):
    return ref.at[pl.ds(pl.multiple_of(start, 64), count)]


def done(ref, sem):
    pltpu.make_async_copy(ref, ref, sem).wait()


STEPS = (
    "10", "01", "02", "20", "03", "bz:0", "wp:0", "fwd:0",
    "11", "T:0", "bz:1", "12", "13", "21", "T:1", "T:-1",
    "far:0", "fz:0", "fz:1", "22", "near:0", "23", "add:0", "adb:0",
    "30", "T:2", "T:-2", "31", "add:1", "add:-1", "adb:1", "adb:-1",
    "32", "sum:0", "33", "T:-3", "T:3", "40", "41", "42",
    "add:-2", "add:2", "adb:-2", "adb:2", "43", "T:4",
)
TAIL = (
    "z:0", "z:1", "sum:1", "sum:-1", "add:-3", "add:3", "adb:-3", "adb:3",
    "sum:-2", "sum:2", "add:4", "adb:4", "sum:-3", "sum:3", "near:1", "sum:4",
    "far:1", "hd:0", "dw:0", "dw:1", "dw:2", "own:0", "own:1", "own:-1",
    "own:2", "own:-2", "own:-3", "own:3", "own:4", "dw:3", "dw:4", "dw:5",
    "dw:6",
)


def kernel(
    hid_in, up_in, w_in, ig_out, dw_out,
    U, UP, H, W, WP, T, c1p, c1m, c2p, c2m, zs, zr, own,
    s_loc, s_a1, s_yp, s_ym, s_up, s_w, s_bz, s_bxp, s_bxm, s_bf, s_bfz, s_hd,
    s_c1p, s_c1m, s_c2p, s_c2m, s_z,
    t_u, t_up, t_w, t_h, t_hd, t_c,
):
    c = lax.axis_index("dp")
    x = lax.axis_index("x")
    h = lax.axis_index("zh")
    y = lax.axis_index("y")
    l = lax.axis_index("zl")
    other = {"dp": 1 - c}
    xp = {"x": lax.rem(x + 1, 4)}
    xm = {"x": lax.rem(x + 3, 4)}
    yp = {"y": lax.rem(y + 1, 8)}
    ym = {"y": lax.rem(y + 7, 8)}
    zo = {"zh": 1 - h}
    line = [l, l + 1 - 2 * lax.rem(l, 2), lax.rem(l + 2, 4), 3 - l]
    mates = [{"zl": k} for k in line[1:]]

    def send(src, dst, t, s, to):
        pltpu.make_async_remote_copy(
            src_ref=src, dst_ref=dst, send_sem=t, recv_sem=s, device_id=to, device_id_type=MESH
        ).start()

    def urow(block, i):
        return (block * 4 + line[i]) * 64

    def hrow(core, xx, hh):
        return (core * 8 + xx * 2 + hh) * 128

    local_up = pltpu.make_async_copy(up_in, rows(U, urow(y, 0), 64), s_loc.at[0])
    local_hid = pltpu.make_async_copy(hid_in, rows(H, hrow(c, x, h), 128), s_loc.at[1])
    local_w = pltpu.make_async_copy(w_in, W, s_loc.at[2])
    local_up.start()
    local_hid.start()
    local_w.start()

    barrier = pltpu.get_barrier_semaphore()
    partners = mates + [yp, ym, xp, xm, zo, other]
    for to in partners:
        pl.semaphore_signal(barrier, inc=1, device_id=to, device_id_type=MESH)
    with jax.named_scope('barrier'):
        pl.semaphore_wait(barrier, len(partners))

    with jax.named_scope('lup'):
        local_up.wait()
    mine = rows(U, urow(y, 0), 64)
    for i in range(1, 4):
        send(mine, mine, t_u, s_a1.at[i - 1], mates[i - 1])

    def to_partner(block, i):
        @pl.when(block // 4 != c)
        def _():
            b4 = lax.rem(block, 4)
            send(rows(U, urow(block, i), 64), rows(UP, (b4 * 4 + line[i]) * 64, 64), t_up, s_up.at[b4], other)

    to_partner(y, 0)
    send(mine, mine, t_u, s_yp.at[0], yp)
    send(mine, mine, t_u, s_ym.at[0], ym)

    with jax.named_scope('lhid'):
        local_hid.wait()

    def share(xx, hh, part, to, sem):
        piece = rows(H, hrow(c, xx, hh) + part * 64, 64)
        send(piece, piece, t_h, sem, to)

    share(x, h, 0, xp, s_bxp.at[0, 0])
    share(x, h, 1, xm, s_bxm.at[0, 1])
    share(x, h, 1, xp, s_bxp.at[0, 1])
    share(x, h, 0, xm, s_bxm.at[0, 0])

    def hid_across(xx, hh):
        piece = rows(H, hrow(c, xx, hh), 128)
        send(piece, piece, t_hd, s_hd.at[0], other)

    hid_across(x, h)
    with jax.named_scope('lw'):
        local_w.wait()
    send(W, WP, t_w, s_w.at[0], other)

    wp = rows(WP, 0, 896)

    def quarter(xx, hh, ab):
        return T.at[xx, pl.ds(pl.multiple_of(hh * 128 + ab * 64, 64), 64)]

    sides = (1 - h, h)

    def place_of(delta):
        block = lax.rem(y + delta + 8, 8)
        b4 = lax.rem(block, 4)
        return block, b4, block // 4 == c, lax.rem(b4 - x + 4, 4)

    def spread(delta):
        _, b4, here, d = place_of(delta)

        @pl.when(jnp.logical_and(here, d == 2))
        def _():
            for k in range(2):
                send(quarter(b4, sides[k], 0), c1p.at[k], t_c, s_c1p.at[k], xp)
                send(quarter(b4, sides[k], 1), c1m.at[k], t_c, s_c1m.at[k], xm)

        @pl.when(jnp.logical_and(here, d == 1))
        def _():
            for k in range(2):
                send(quarter(b4, sides[k], 1), c2p.at[k, 1], t_c, s_c2p.at[k, 1], xp)

        @pl.when(jnp.logical_and(here, d == 3))
        def _():
            for k in range(2):
                send(quarter(b4, sides[k], 0), c2m.at[k, 0], t_c, s_c2m.at[k, 0], xm)

    def block_step(delta):
        block, b4, here, d = place_of(delta)

        @pl.when(here)
        def _():
            done(rows(UP, b4 * 256, 256), s_up.at[b4])
            u = rows(U, block * 256, 256)
            up = rows(UP, b4 * 256, 256)
            dims = (((1,), (1,)), ((), ()))
            for n0 in range(0, 896, 256):
                n1 = min(n0 + 256, 896)
                acc = lax.dot_general(u[...], W[n0:n1], dims, preferred_element_type=F32)
                acc += lax.dot_general(up[...], WP[n0:n1], dims, preferred_element_type=F32)
                T[b4, :, n0:n1] = acc.astype(BF16)

        spread(delta)

    def add_step(delta, k):
        _, b4, here, d = place_of(delta)

        @pl.when(jnp.logical_and(here, d == 1))
        def _():
            done(c1p.at[k], s_c1p.at[k])
            q = quarter(b4, sides[k], 0)
            q[...] = (q[...].astype(F32) + c1p[k].astype(F32)).astype(BF16)
            send(q, c2p.at[k, 0], t_c, s_c2p.at[k, 0], xp)

        @pl.when(jnp.logical_and(here, d == 3))
        def _():
            done(c1m.at[k], s_c1m.at[k])
            q = quarter(b4, sides[k], 1)
            q[...] = (q[...].astype(F32) + c1m[k].astype(F32)).astype(BF16)
            send(q, c2m.at[k, 1], t_c, s_c2m.at[k, 1], xm)

    def sum_step(delta, k):
        _, b4, here, d = place_of(delta)

        @pl.when(jnp.logical_and(here, d == 0))
        def _():
            for p in (1, 0):
                done(c2p.at[k, p], s_c2p.at[k, p])
                done(c2m.at[k, p], s_c2m.at[k, p])
                total = quarter(b4, sides[k], p)[...].astype(F32) + c2p[k, p].astype(F32) + c2m[k, p].astype(F32)
                if k == 0:
                    zs[p] = total.astype(BF16)
                    send(zs.at[p], zr.at[p], t_c, s_z.at[p], zo)
                else:
                    own[p] = total

    def last_step():
        for p in range(2):
            done(zr.at[p], s_z.at[p])
            ig_out[p * 64 : p * 64 + 64] = (own[p] + zr[p].astype(F32)).astype(BF16)

    def forward(hh, e):
        left, right = lax.rem(x + 3, 4), lax.rem(x + 1, 4)
        done(rows(H, hrow(c, left, hh), 64), s_bxp.at[e, 0])
        share(left, hh, 0, xp, s_bf.at[0])
        done(rows(H, hrow(c, right, hh) + 64, 64), s_bxm.at[e, 1])
        share(right, hh, 1, xm, s_bf.at[1])

    def across_near(hh, e):
        left, right = lax.rem(x + 3, 4), lax.rem(x + 1, 4)
        for part in (0, 1) if e == 1 else (1,):
            done(rows(H, hrow(c, left, hh) + part * 64, 64), s_bxp.at[e, part])
        hid_across(left, hh)
        for part in (1, 0) if e == 1 else (0,):
            done(rows(H, hrow(c, right, hh) + part * 64, 64), s_bxm.at[e, part])
        hid_across(right, hh)

    def across_far(hh, e):
        far = lax.rem(x + 2, 4)
        s_a, s_b = (s_bf.at[0], s_bf.at[1]) if e == 0 else (s_bfz.at[0], s_bfz.at[1])
        done(rows(H, hrow(c, far, hh), 64), s_a)
        done(rows(H, hrow(c, far, hh) + 64, 64), s_b)
        hid_across(far, hh)

    def far_along_z(part):
        share(lax.rem(x + 2, 4), h, part, zo, s_bfz.at[part])

    def from_z(part):
        done(rows(H, hrow(c, x, 1 - h) + part * 64, 64), s_bz.at[part])
        first, second = (xp, xm) if part == 0 else (xm, xp)
        share(x, 1 - h, part, xp, s_bxp.at[1, part])
        share(x, 1 - h, part, xm, s_bxm.at[1, part])
        if part == 1:
            hid_across(x, 1 - h)

    def halves():
        done(rows(H, (1 - c) * 1024, 1024), s_hd.at[0])

    def dw_tile(f):
        cols = slice(f * 128, f * 128 + 128)
        dw_out[cols] = lax.dot_general(H[:, cols], U[...], (((0,), (0,)), ((), ())), preferred_element_type=F32)

    ways = {
        "T": block_step,
        "add": lambda delta: add_step(delta, 0),
        "adb": lambda delta: add_step(delta, 1),
        "sum": lambda delta: sum_step(delta, 0),
        "own": lambda delta: sum_step(delta, 1),
        "dw": dw_tile,
        "z": from_z,
        "bz": lambda p: share(x, h, p, zo, s_bz.at[p]),
        "fwd": lambda _: forward(h, 0),
        "fz": far_along_z,
        "near": lambda e: across_near((h, 1 - h)[e], e),
        "far": lambda e: across_far((h, 1 - h)[e], e),
        "hd": lambda _: halves(),
        "wp": lambda _: done(wp, s_w.at[0]),
    }

    def run(line_of_tasks):
        for task in line_of_tasks:
            name, number = task.split(":")
            with jax.named_scope(task.replace(":", "_").replace("-", "m")):
                ways[name](int(number))

    def onward(k, i):
        if k == 0:
            piece = rows(U, urow(y, i), 64)
            with jax.named_scope(f"a1_{i}"):
                done(piece, s_a1.at[i - 1])
            send(piece, piece, t_u, s_yp.at[i], yp)
            send(piece, piece, t_u, s_ym.at[i], ym)
            to_partner(y, i)
            return
        n = k * 4 + i
        for block, sem, to, last in (
            (lax.rem(y - k + 8, 8), s_yp, yp, (0, 1)),
            (lax.rem(y + k, 8), s_ym, ym, (2, 3)),
        ):
            if k == 4 and i not in last:
                continue
            piece = rows(U, urow(block, i), 64)
            with jax.named_scope(f"y{k}_{i}"):
                done(piece, sem.at[n - 4])
            if k < 3 or (k == 3 and i in last):
                send(piece, piece, t_u, sem.at[n], to)
            to_partner(block, i)

    for step in STEPS:
        if ":" in step:
            run((step,))
        else:
            onward(int(step[0]), int(step[1]))
    run(TAIL)
    with jax.named_scope('last'):
        last_step()

    with jax.named_scope('fin'):
        done(rows(U, 0, 1984), t_u)
    done(UP, t_up)
    done(W, t_w)
    done(rows(H, 0, 1024), t_hd)
    done(rows(H, 0, 896), t_h)
    done(rows(H, 0, 896), t_c)


def put_out(grad, weight_grad, grad_out, weight_grad_out, sems):
    copies = [pltpu.make_async_copy(grad, grad_out, sems.at[7])]
    for f in range(7):
        part = pl.ds(f * 128, 128)
        copies.append(pltpu.make_async_copy(weight_grad.at[part], weight_grad_out.at[part], sems.at[f]))
    for copy in copies:
        copy.start()
    for copy in copies:
        copy.wait()


def local(hidden, upstream, weight):
    dma = pltpu.SemaphoreType.DMA
    hidden, upstream, weight = (pltpu.with_memory_space_constraint(a, pltpu.HBM) for a in (hidden, upstream, weight))
    grad, weight_grad = pl.pallas_call(
        kernel,
        out_shape=(jax.ShapeDtypeStruct((128, 896), BF16), jax.ShapeDtypeStruct((896, 512), F32)),
        in_specs=[pl.BlockSpec(memory_space=pltpu.HBM)] * 3,
        out_specs=[pl.BlockSpec(memory_space=pltpu.VMEM)] * 2,
        scratch_shapes=[
            pltpu.VMEM((2048, 512), BF16),
            pltpu.VMEM((1024, 512), BF16),
            pltpu.VMEM((2048, 896), BF16),
            pltpu.VMEM((896, 512), BF16),
            pltpu.VMEM((896, 512), BF16),
            pltpu.VMEM((4, 256, 896), BF16),
            pltpu.VMEM((2, 64, 896), BF16),
            pltpu.VMEM((2, 64, 896), BF16),
            pltpu.VMEM((2, 2, 64, 896), BF16),
            pltpu.VMEM((2, 2, 64, 896), BF16),
            pltpu.VMEM((2, 64, 896), BF16),
            pltpu.VMEM((2, 64, 896), BF16),
            pltpu.VMEM((2, 64, 896), F32),
            dma((3,)), dma((3,)), dma((16,)), dma((16,)), dma((4,)), dma((1,)), dma((2,)),
            dma((2, 2)), dma((2, 2)), dma((2,)), dma((2,)), dma((1,)),
            dma((2,)), dma((2,)), dma((2, 2)), dma((2, 2)), dma((2,)),
            dma, dma, dma, dma, dma, dma,
        ],
        compiler_params=pltpu.CompilerParams(
            collective_id=0, has_side_effects=True, vmem_limit_bytes=40 << 20
        ),
    )(hidden, upstream, weight)
    return pl.pallas_call(
        put_out,
        out_shape=(pltpu.HBM((128, 896), BF16), pltpu.HBM((896, 512), F32)),
        in_specs=[pl.BlockSpec(memory_space=pltpu.VMEM)] * 2,
        out_specs=[pl.BlockSpec(memory_space=pltpu.HBM)] * 2,
        scratch_shapes=[dma((8,))],
        compiler_params=pltpu.CompilerParams(vmem_limit_bytes=8 << 20),
    )(*(pltpu.with_memory_space_constraint(a, pltpu.VMEM) for a in (grad, weight_grad)))


def solution(mesh):
    finer = Mesh(mesh.devices.reshape(2, 4, 2, 8, 4), ("dp", "x", "zh", "y", "zl"))
    placed = (P(DP_ROW, COL), P(COL, DP_ROW), P(COL, DP_ROW))
    return jax.shard_map(
        local,
        mesh=finer,
        in_specs=placed,
        out_specs=(P(DP_ROW, COL), P(COL, DP_ROW)),
        check_vma=False,
    )
```
